256 devices in a mesh: grp: 16 (over z, core), reg: 16 (over y, x).
Axes of the slice: x: 4, y: 4, z: 8, core: 2. Of those that a mesh axis runs over, the one named last changes fastest.
Arguments:
- queries: bfloat16 [32768, 1536], P(('grp', 'reg')), parts along dimension 0, may hold values from -9 to 9
- keys_now: bfloat16 [32768, 1536], P(('grp', 'reg')), parts along dimension 0, may hold values from -9 to 9
- values_now: bfloat16 [32768, 1536], P(('grp', 'reg')), parts along dimension 0, may hold values from -6 to 6
- keys_stale: bfloat16 [32768, 1536], P(('grp', 'reg')), parts along dimension 0, may hold values from -9 to 9
- values_stale: bfloat16 [32768, 1536], P(('grp', 'reg')), parts along dimension 0, may hold values from -6 to 6
- neighbours: int32 [256, 8], P('grp'), parts along dimension 0, may hold values from -1 to 15, as said below
Outputs:
- attended: bfloat16 [32768, 1536], P(('grp', 'reg')), parts along dimension 0
The draws below stay inside these ranges and needn't reach their ends.
There are 16 independent parts, one for each index of `grp`. The reference program is written for one: setup_inputs(seed, part) draws one part's arguments, and reference() takes and returns one part's arrays. A program takes and returns all parts, laid end to end along the dimension named above; each array names one. Nothing has to cross between parts.
Inputs may be any that keep to these rules, and one draw needn't show every extreme that they name: `neighbours`: row r holds first between 1 and 8 distinct region numbers other than r, then -1 in its remaining slots; some row holds 8 numbers.
All inputs are finite; a program needn't handle non-finite values.
Results may differ from the reference program's by a relative error of at most 0.0085.
Values may be sent and summed in bfloat16 or wider, within the bound.
A program may use at most 128 MiB of HBM per device.

```python
import jax
import jax.numpy as jnp
from jax import lax

HEADS = 12
HD = 128
TOK_DEV = 128
HALO = 128
TOKENS = 2048
F = 1536
N_REG = 16


def neighbour_table(key):
    base = jax.random.fold_in(key, 777)
    key_perm, key_long, key_base = jax.random.split(base, 3)
    slot_count = N_REG // 2

    def one_row(region):
        shuffled = jax.random.permutation(jax.random.fold_in(key_perm, region), N_REG)
        order = jnp.argsort((shuffled == region).astype(jnp.int32), stable=True)
        return shuffled[order][:slot_count]
    lists = jax.vmap(one_row)(jnp.arange(N_REG, dtype=jnp.int32))
    longest = jax.random.randint(key_long, (2,), 0, N_REG)
    counts = 1 + jax.random.randint(key_base, (N_REG,), 0, 2)
    counts = jnp.minimum(counts, slot_count).at[longest].set(slot_count)
    columns = jnp.arange(slot_count, dtype=jnp.int32)
    return jnp.where(columns[None, :] < counts[:, None], lists, -1).astype(jnp.int32)


def joint_draw(key):
    base = jax.random.fold_in(key, 4242)
    key_query = jax.random.fold_in(base, 0)
    key_keys = jax.random.fold_in(base, 1)
    key_stale = jax.random.fold_in(base, 5)
    width = HEADS * HD
    total_rows = TOK_DEV * N_REG
    query_vals = 1.5 * jnp.clip(jax.random.normal(key_query, (total_rows, width), jnp.float32), -6.0, 6.0)
    key_vals = jnp.clip(jax.random.normal(key_keys, (total_rows, width), jnp.float32), -6.0, 6.0)
    stale_vals = jnp.clip(jax.random.normal(key_stale, (total_rows, width), jnp.float32), -6.0, 6.0)
    return (query_vals, key_vals, stale_vals)


def draw_queries(key, part):
    return joint_draw(key)[0].astype(jnp.bfloat16)


def draw_keys_now(key, part):
    return joint_draw(key)[1].astype(jnp.bfloat16)


def draw_keys_stale(key, part):
    return joint_draw(key)[2].astype(jnp.bfloat16)


def draw_neighbours(key, part):
    return neighbour_table(key)


def block_levels(stream_key, shape, cuts, low, top_value):
    gain = 1.0
    for axis_at, blocks in cuts:
        steps = jax.random.uniform(jax.random.fold_in(jax.random.fold_in(stream_key, 6), axis_at), (blocks,), jnp.float32, low / len(cuts), top_value / len(cuts))
        gain = gain * jnp.repeat(jnp.exp(steps), shape[axis_at] // blocks).reshape((-1,) + (1,) * (len(shape) - 1 - axis_at))
    return gain


def centred(rng, shape, spread, limit, cuts=(), kind=jnp.bfloat16):
    level = block_levels(rng, shape, cuts, -0.22, 0.18) if cuts else 1.0
    drawn = jax.random.normal(rng, shape, jnp.float32) * spread * level
    return jnp.minimum(jnp.maximum(drawn, -limit), limit).astype(kind)


def setup_inputs(seed: int = 0, part: int = 0) -> dict:
    key_of = jax.random.split(jax.random.key(seed), 7)
    part_keys = jax.random.split(jax.random.fold_in(key_of[6], part), 7)
    return {
        "queries": draw_queries(jax.random.fold_in(jax.random.fold_in(key_of[6], part), 71), part),
        "keys_now": draw_keys_now(jax.random.fold_in(jax.random.fold_in(key_of[6], part), 71), part),
        "values_now": centred(part_keys[2], (TOKENS, F), 1.0, 6.0, ((0, 16),)),
        "keys_stale": draw_keys_stale(jax.random.fold_in(jax.random.fold_in(key_of[6], part), 71), part),
        "values_stale": centred(part_keys[4], (TOKENS, F), 1.0, 6.0, ((0, 16),)),
        "neighbours": draw_neighbours(jax.random.fold_in(jax.random.fold_in(key_of[6], part), 71), part),
    }


def block_partial(query_rows, key_rows, value_rows, key_valid):
    rows = query_rows.shape[0]
    count = key_rows.shape[0]
    query3 = query_rows.reshape(rows, HEADS, HD).astype(jnp.float32)
    key3 = key_rows.reshape(count, HEADS, HD).astype(jnp.float32)
    value3 = value_rows.reshape(count, HEADS, HD).astype(jnp.float32)
    scores = jnp.einsum('thd,shd->ths', query3, key3) * (HD ** -0.5)
    scores = jnp.where(key_valid[None, None, :], scores, -jnp.inf)
    peak = jnp.max(scores, axis=-1)
    weights = jnp.exp(scores - peak[..., None])
    total = jnp.sum(weights, axis=-1)
    rounded = weights.astype(jnp.bfloat16).astype(jnp.float32)
    numer = jnp.einsum('ths,shd->thd', rounded, value3)
    partial_out = (numer / total[..., None]).reshape(rows, HEADS * HD).astype(jnp.bfloat16)
    return peak, total, partial_out


def reference(queries, keys_now, values_now, keys_stale, values_stale, neighbours):
    total_rows = TOK_DEV * N_REG
    span = TOK_DEV + 2 * HALO
    keys_pad = jnp.pad(keys_now, ((HALO, HALO), (0, 0)))
    values_pad = jnp.pad(values_now, ((HALO, HALO), (0, 0)))
    owners = jnp.arange(N_REG, dtype=jnp.int32)

    def one_region(region):
        start = (region * TOK_DEV).astype(jnp.int32)
        query_rows = lax.dynamic_slice_in_dim(queries, start, TOK_DEV, 0)
        local_keys = lax.dynamic_slice_in_dim(keys_pad, start, span, 0)
        local_values = lax.dynamic_slice_in_dim(values_pad, start, span, 0)
        position = start - HALO + jnp.arange(span, dtype=jnp.int32)
        valid = (position >= 0) & (position < total_rows)
        peak_local, total_local, out_local = block_partial(query_rows, local_keys, local_values, valid)
        own_list = neighbours[region]
        member = jnp.any(own_list[:, None] == owners[None, :], axis=0)

        def one_owner(owner):
            begin = (owner * TOK_DEV).astype(jnp.int32)
            key_rows = lax.dynamic_slice_in_dim(keys_stale, begin, TOK_DEV, 0)
            value_rows = lax.dynamic_slice_in_dim(values_stale, begin, TOK_DEV, 0)
            return block_partial(query_rows, key_rows, value_rows, jnp.ones((TOK_DEV,), bool))

        peaks, totals, outs = lax.map(one_owner, owners)
        masked_peaks = jnp.where(member[:, None, None], peaks, -jnp.inf)
        top = jnp.maximum(peak_local, jnp.max(masked_peaks, axis=0))
        weight_local = jnp.exp(peak_local - top) * total_local
        weights = jnp.where(member[:, None, None], jnp.exp(masked_peaks - top) * totals, 0.0)
        denom = weight_local + jnp.sum(weights, axis=0)
        numer = weight_local[..., None] * out_local.astype(jnp.float32).reshape(TOK_DEV, HEADS, HD)
        numer = numer + jnp.einsum('nth,nthd->thd', weights, outs.astype(jnp.float32).reshape(N_REG, TOK_DEV, HEADS, HD))
        return (numer / denom[..., None]).reshape(TOK_DEV, HEADS * HD).astype(jnp.bfloat16)

    result = lax.map(one_region, owners)
    return result.reshape(total_rows, HEADS * HD)
```

```python
import functools

import jax
import jax.numpy as jnp
from jax import lax
from jax.experimental import pallas as pl
from jax.experimental.pallas import tpu as pltpu
from jax.sharding import PartitionSpec as P

HD = 128
MESH = pl.DeviceIdType.MESH
LOG2E = 1.4426950408889634
LOW = -1e30
ORDER = (
    (0, 1), (0, 3), (1, 0), (3, 0), (1, 1), (3, 3), (1, 3), (3, 1),
    (2, 0), (0, 2), (2, 1), (3, 2), (2, 3), (1, 2), (2, 2),
)


def kernel(side, slots, nb_ref, q_ref, ks_ref, kn_ref, vs_ref, vn_ref, out_ref,
           stage, in_q, in_ks, in_kn, in_vs, in_vn, ps, pn, mb, lb, osum, outbox,
           load_sem, send_sem, recv_sem, osend_sem, orecv_sem):
    n = side * side
    per = side - 1
    heads = per * side
    rows = q_ref.shape[0]
    core = lax.rem(lax.axis_index("grp"), 2)
    me = lax.axis_index("reg")
    y, x = me // side, lax.rem(me, side)
    scale = HD ** -0.5 * LOG2E

    def place(dy, dx):
        yy, xx = lax.rem(y + dy, side), lax.rem(x + dx, side)
        kk = lax.rem(xx + yy + 2 * core, side)
        return yy * side + xx, yy * per + kk, kk < per

    _, my_head, active = place(0, 0)
    args = (q_ref, ks_ref, kn_ref, vs_ref, vn_ref)
    inbox = (in_q, in_ks, in_kn, in_vs, in_vn)

    def cols(h):
        return pl.ds(pl.multiple_of(h * HD, HD), HD)

    for t, ref in enumerate(args):
        pltpu.make_async_copy(ref, stage.at[t], load_sem.at[t]).start()

    barrier = pltpu.get_barrier_semaphore()
    for o in range(1, n):
        pl.semaphore_signal(barrier, inc=1, device_id={"reg": lax.rem(me + o, n)}, device_id_type=MESH)

    @pl.when(active)
    def _():
        for t, ref in enumerate(args):
            pltpu.make_async_copy(ref.at[:, cols(my_head)], inbox[t].at[me], recv_sem.at[t]).start()

    pl.semaphore_wait(barrier, n - 1)

    for t, ref in enumerate(args):
        pltpu.make_async_copy(ref, stage.at[t], load_sem.at[t]).wait()
        for dy, dx in ORDER:
            dev, head, owns = place(dy, dx)

            @pl.when(owns)
            def _():
                pltpu.make_async_remote_copy(
                    src_ref=stage.at[t, :, cols(head)],
                    dst_ref=inbox[t].at[me],
                    send_sem=send_sem.at[t],
                    recv_sem=recv_sem.at[t],
                    device_id={"reg": dev},
                    device_id_type=MESH,
                ).start()

    def arrived(t):
        pltpu.make_async_copy(inbox[t], inbox[t], recv_sem.at[t]).wait()

    def softmax_parts(scores):
        peak = jnp.max(scores, axis=-1, keepdims=True)
        weights = jnp.exp2((scores - peak) * scale)
        total = jnp.sum(weights, axis=-1, keepdims=True)
        return peak, weights, total

    @pl.when(active)
    def _():
        arrived(0)
        arrived(1)

        def stale_scores(r, _):
            q = in_q[r]
            idx = [nb_ref[s, r] for s in range(slots)]
            keys = jnp.concatenate([in_ks[jnp.maximum(i, 0)] for i in idx], axis=0)
            sc = lax.dot_general(q, keys, (((1,), (1,)), ((), ())), preferred_element_type=jnp.float32)
            sc = jnp.concatenate(
                [jnp.where(i >= 0, sc[:, s * rows:(s + 1) * rows], LOW) for s, i in enumerate(idx)], axis=1)
            peak, weights, total = softmax_parts(sc)
            ps[r] = weights.astype(jnp.bfloat16)
            mb[r] = jnp.broadcast_to(peak, (rows, HD))
            lb[r] = jnp.broadcast_to(total, (rows, HD))
            return 0

        lax.fori_loop(0, n, stale_scores, 0)
        arrived(2)

        def local_scores(r, _):
            q = in_q[r]
            keys = jnp.concatenate(
                [in_kn[jnp.maximum(r - 1, 0)], in_kn[r], in_kn[jnp.minimum(r + 1, n - 1)]], axis=0)
            sc = lax.dot_general(q, keys, (((1,), (1,)), ((), ())), preferred_element_type=jnp.float32)
            sc = jnp.concatenate([
                jnp.where(r > 0, sc[:, :rows], LOW),
                sc[:, rows:2 * rows],
                jnp.where(r < n - 1, sc[:, 2 * rows:], LOW)], axis=1)
            peak, weights, total = softmax_parts(sc)
            peak_s, total_s = mb[r], lb[r]
            peak = jnp.broadcast_to(peak, (rows, HD))
            top = jnp.maximum(peak, peak_s)
            keep_n = jnp.exp2((peak - top) * scale)
            keep_s = jnp.exp2((peak_s - top) * scale)
            inv = 1.0 / (keep_n * total + keep_s * total_s)
            lb[r] = keep_s * inv
            wn = keep_n * inv
            pn[r] = (weights * jnp.concatenate([wn, wn, wn], axis=1)).astype(jnp.bfloat16)
            return 0

        lax.fori_loop(0, n, local_scores, 0)
        arrived(3)

        def stale_values(r, _):
            values = jnp.concatenate(
                [in_vs[jnp.maximum(nb_ref[s, r], 0)] for s in range(slots)], axis=0)
            osum[r] = lb[r] * jnp.dot(ps[r], values, preferred_element_type=jnp.float32)
            return 0

        lax.fori_loop(0, n, stale_values, 0)
        arrived(4)

        def tile(r):
            values = jnp.concatenate(
                [in_vn[jnp.maximum(r - 1, 0)], in_vn[r], in_vn[jnp.minimum(r + 1, n - 1)]], axis=0)
            return (osum[r] + jnp.dot(pn[r], values, preferred_element_type=jnp.float32)).astype(jnp.bfloat16)

        def finish(o, _):
            r = lax.rem(me + o, n)
            outbox[r] = tile(r)
            pltpu.make_async_remote_copy(
                src_ref=outbox.at[r],
                dst_ref=out_ref.at[:, cols(my_head)],
                send_sem=osend_sem,
                recv_sem=orecv_sem,
                device_id={"reg": r},
                device_id_type=MESH,
            ).start()
            return 0

        lax.fori_loop(1, n, finish, 0)
        out_ref[:, cols(my_head)] = tile(me)

    def spent(count):
        for t in range(len(args)):
            part = stage.at[t, :, pl.ds(0, count * HD)]
            pltpu.make_async_copy(part, part, send_sem.at[t]).wait()
        got = out_ref.at[:, pl.ds(0, count * HD)]
        pltpu.make_async_copy(got, got, orecv_sem).wait()

    @pl.when(active)
    def _():
        spent(heads - 1)
        sent = outbox.at[pl.ds(0, n - 1)]
        pltpu.make_async_copy(sent, sent, osend_sem).wait()

    @pl.when(jnp.logical_not(active))
    def _():
        spent(heads)


def solution(mesh):
    n = mesh.shape["reg"]
    side = 4
    assert side * side == n

    def on_device(queries, keys_now, values_now, keys_stale, values_stale, neighbours):
        rows, width = queries.shape
        slots = neighbours.shape[1]
        any_spec = pl.BlockSpec(memory_space=pl.ANY)
        return pl.pallas_call(
            functools.partial(kernel, side, slots),
            out_shape=jax.ShapeDtypeStruct((rows, width), jnp.bfloat16),
            in_specs=[pl.BlockSpec(memory_space=pltpu.SMEM)] + [any_spec] * 5,
            out_specs=pl.BlockSpec(memory_space=pltpu.VMEM),
            scratch_shapes=[
                pltpu.VMEM((5, rows, width), jnp.bfloat16),
            ] + [pltpu.VMEM((n, rows, HD), jnp.bfloat16)] * 5 + [
                pltpu.VMEM((n, rows, slots * rows), jnp.bfloat16),
                pltpu.VMEM((n, rows, 3 * rows), jnp.bfloat16),
                pltpu.VMEM((n, rows, HD), jnp.float32),
                pltpu.VMEM((n, rows, HD), jnp.float32),
                pltpu.VMEM((n, rows, HD), jnp.float32),
                pltpu.VMEM((n, rows, HD), jnp.bfloat16),
                pltpu.SemaphoreType.DMA((5,)),
                pltpu.SemaphoreType.DMA((5,)),
                pltpu.SemaphoreType.DMA((5,)),
                pltpu.SemaphoreType.DMA,
                pltpu.SemaphoreType.DMA,
            ],
            compiler_params=pltpu.CompilerParams(collective_id=0, has_side_effects=True),
        )(neighbours.T, queries, keys_stale, keys_now, values_stale, values_now)

    in_specs = (P(("grp", "reg"), None),) * 5 + (P("grp", None),)
    return jax.shard_map(
        on_device, mesh=mesh, in_specs=in_specs, out_specs=P(("grp", "reg"), None), check_vma=False
    )
```

```python
import functools

import jax
import jax.numpy as jnp
from jax import lax
from jax.experimental import pallas as pl
from jax.experimental.pallas import tpu as pltpu
from jax.sharding import PartitionSpec as P

HD = 128
MESH = pl.DeviceIdType.MESH
LOG2E = 1.4426950408889634
LOW = -1e30
GROUP = 4
Q, KS, KN, VS, VN = range(5)
ORDER = (
    (0, 1), (0, 3), (1, 0), (3, 0), (1, 1), (3, 3), (1, 3), (3, 1),
    (2, 0), (0, 2), (2, 1), (3, 2), (2, 3), (1, 2), (2, 2),
)


def kernel(side, slots, nb_ref, q_ref, ks_ref, kn_ref, vs_ref, vn_ref, out_ref,
           stage, in_q, in_ks, in_kn, in_vs, in_vn, ps, pn, mb, lb, osum, outbox,
           load_sem, send_sem, recv_sem, fsend_sem, frecv_sem, osend_sem, orecv_sem):
    n = side * side
    half = n // 2
    rows = q_ref.shape[0]
    core = lax.rem(lax.axis_index("grp"), 2)
    me = lax.axis_index("reg")
    y, x = me // side, lax.rem(me, side)
    part = y // 2
    scale = HD ** -0.5 * LOG2E
    args = (q_ref, ks_ref, kn_ref, vs_ref, vn_ref)
    inbox = (in_q, in_ks, in_kn, in_vs, in_vn)

    def role(yy, xx):
        whole = lax.rem(xx + core, 2) == 0
        outer = (yy // (side - 1) + (side - 1 - yy) // (side - 1)).astype(jnp.int32)
        return whole, jnp.where(whole, yy * 2 + xx // 2, n // 2 + 2 * outer + xx // 2)

    whole, my_head = role(y, x)
    shared = jnp.logical_not(whole)
    partner = (side - 1 - y) * side + x
    edge = jnp.logical_or(me == half - 1, me == half)
    first = jnp.where(whole, 0, part * half)
    count = jnp.where(whole, n, half)

    def cols(h):
        return pl.ds(pl.multiple_of(h * HD, HD), HD)

    for t, ref in enumerate(args):
        pltpu.make_async_copy(ref, stage.at[t], load_sem.at[t]).start()
    for t, ref in enumerate(args):
        pltpu.make_async_copy(ref.at[:, cols(my_head)], inbox[t].at[me], recv_sem.at[t]).start()

    barrier = pltpu.get_barrier_semaphore()
    for o in range(1, n):
        pl.semaphore_signal(barrier, inc=1, device_id={"reg": lax.rem(me + o, n)}, device_id_type=MESH)
    pl.semaphore_wait(barrier, n - 1)

    def send(t):
        pltpu.make_async_copy(args[t], stage.at[t], load_sem.at[t]).wait()
        for dy, dx in ORDER:
            yy, xx = lax.rem(y + dy, side), lax.rem(x + dx, side)
            takes, head = role(yy, xx)
            takes = jnp.logical_or(takes, yy // 2 == part)
            if t in (KN, VN):
                takes = jnp.logical_or(takes, edge)

            @pl.when(takes)
            def _():
                pltpu.make_async_remote_copy(
                    src_ref=stage.at[t, :, cols(head)],
                    dst_ref=inbox[t].at[me],
                    send_sem=send_sem.at[t],
                    recv_sem=recv_sem.at[t],
                    device_id={"reg": yy * side + xx},
                    device_id_type=MESH,
                ).start()

    def wait(sem, tiles):
        some = in_q.at[pl.ds(0, tiles)]
        pltpu.make_async_copy(some, some, sem).wait()

    most = n - 1 - side

    def sent(t):
        if t in (KN, VN):
            @pl.when(edge)
            def _():
                wait(send_sem.at[t], n - 1)

            @pl.when(jnp.logical_not(edge))
            def _():
                wait(send_sem.at[t], most)
        else:
            wait(send_sem.at[t], most)

    def arrived(t):
        @pl.when(whole)
        def _():
            wait(recv_sem.at[t], n)

        @pl.when(shared)
        def _():
            wait(recv_sem.at[t], half + 1 if t in (KN, VN) else half)

    def forward(t):
        mine = inbox[t].at[pl.ds(part * half, half)]
        return pltpu.make_async_remote_copy(
            src_ref=mine,
            dst_ref=mine,
            send_sem=fsend_sem.at[t // 2],
            recv_sem=frecv_sem.at[t // 2],
            device_id={"reg": partner},
            device_id_type=MESH,
        )

    def pass_on(t):
        arrived(t)

        @pl.when(shared)
        def _():
            forward(t).start()

    def passed(t):
        @pl.when(shared)
        def _():
            wait(frecv_sem.at[t // 2], half)

    send(KS)
    send(Q)
    sent(KS)
    send(KN)
    pass_on(KS)
    sent(Q)
    send(VS)
    arrived(Q)
    passed(KS)

    def softmax_parts(scores):
        peak = jnp.max(scores, axis=-1, keepdims=True)
        weights = jnp.exp2((scores - peak) * scale)
        total = jnp.sum(weights, axis=-1, keepdims=True)
        return peak, weights, total

    def each(one, *outs):
        def step(i, _):
            at = [first + i * GROUP + k for k in range(GROUP)]
            got = [one(r) for r in at]
            for r, values in zip(at, got):
                for ref, value in zip(outs, values):
                    ref[r] = value
            return 0

        lax.fori_loop(0, count // GROUP, step, 0)

    def stale_scores(r):
        idx = [nb_ref[s, r] for s in range(slots)]
        keys = jnp.concatenate([in_ks[jnp.maximum(i, 0)] for i in idx], axis=0)
        sc = lax.dot_general(in_q[r], keys, (((1,), (1,)), ((), ())), preferred_element_type=jnp.float32)
        sc = jnp.concatenate(
            [jnp.where(i >= 0, sc[:, s * rows:(s + 1) * rows], LOW) for s, i in enumerate(idx)], axis=1)
        peak, weights, total = softmax_parts(sc)
        return weights.astype(jnp.bfloat16), jnp.broadcast_to(peak, (rows, HD)), jnp.broadcast_to(total, (rows, HD))

    each(stale_scores, ps, mb, lb)
    sent(KN)
    send(VN)
    pass_on(VS)
    arrived(KN)

    def around(ref, r):
        return jnp.concatenate([ref[jnp.maximum(r - 1, 0)], ref[r], ref[jnp.minimum(r + 1, n - 1)]], axis=0)

    def local_scores(r):
        sc = lax.dot_general(
            in_q[r], around(in_kn, r), (((1,), (1,)), ((), ())), preferred_element_type=jnp.float32)
        sc = jnp.concatenate([
            jnp.where(r > 0, sc[:, :rows], LOW),
            sc[:, rows:2 * rows],
            jnp.where(r < n - 1, sc[:, 2 * rows:], LOW)], axis=1)
        peak, weights, total = softmax_parts(sc)
        peak_s, total_s = mb[r], lb[r]
        peak = jnp.broadcast_to(peak, (rows, HD))
        top = jnp.maximum(peak, peak_s)
        keep_n = jnp.exp2((peak - top) * scale)
        keep_s = jnp.exp2((peak_s - top) * scale)
        inv = 1.0 / (keep_n * total + keep_s * total_s)
        wn = keep_n * inv
        return (weights * jnp.concatenate([wn, wn, wn], axis=1)).astype(jnp.bfloat16), keep_s * inv

    each(local_scores, pn, lb)
    passed(VS)

    def stale_values(r):
        values = jnp.concatenate([in_vs[jnp.maximum(nb_ref[s, r], 0)] for s in range(slots)], axis=0)
        return (lb[r] * jnp.dot(ps[r], values, preferred_element_type=jnp.float32),)

    each(stale_values, osum)
    arrived(VN)

    def tile(r):
        return (osum[r] + jnp.dot(pn[r], around(in_vn, r), preferred_element_type=jnp.float32)).astype(jnp.bfloat16)

    def finish(o, _):
        r = first + lax.rem(me - first + o, count)
        outbox[r] = tile(r)
        pltpu.make_async_remote_copy(
            src_ref=outbox.at[r],
            dst_ref=out_ref.at[:, cols(my_head)],
            send_sem=osend_sem,
            recv_sem=orecv_sem,
            device_id={"reg": r},
            device_id_type=MESH,
        ).start()
        return 0

    lax.fori_loop(1, count, finish, 0)
    out_ref[:, cols(my_head)] = tile(me)

    sent(VS)
    sent(VN)

    @pl.when(whole)
    def _():
        wait(osend_sem, n - 1)

    @pl.when(shared)
    def _():
        wait(osend_sem, half - 1)
        wait(fsend_sem.at[0], half)
        wait(fsend_sem.at[1], half)

    wait(orecv_sem, most)


def solution(mesh):
    n = mesh.shape["reg"]
    side = 4
    assert side * side == n

    def on_device(queries, keys_now, values_now, keys_stale, values_stale, neighbours):
        rows, width = queries.shape
        slots = neighbours.shape[1]
        assert width == (n - side) * HD
        any_spec = pl.BlockSpec(memory_space=pl.ANY)
        dma = pltpu.SemaphoreType.DMA
        return pl.pallas_call(
            functools.partial(kernel, side, slots),
            out_shape=jax.ShapeDtypeStruct((rows, width), jnp.bfloat16),
            in_specs=[pl.BlockSpec(memory_space=pltpu.SMEM)] + [any_spec] * 5,
            out_specs=pl.BlockSpec(memory_space=pltpu.VMEM),
            scratch_shapes=[pltpu.VMEM((5, rows, width), jnp.bfloat16)]
            + [pltpu.VMEM((n, rows, HD), jnp.bfloat16)] * 5
            + [
                pltpu.VMEM((n, rows, slots * rows), jnp.bfloat16),
                pltpu.VMEM((n, rows, 3 * rows), jnp.bfloat16),
                pltpu.VMEM((n, rows, HD), jnp.float32),
                pltpu.VMEM((n, rows, HD), jnp.float32),
                pltpu.VMEM((n, rows, HD), jnp.float32),
                pltpu.VMEM((n, rows, HD), jnp.bfloat16),
                dma((5,)), dma((5,)), dma((5,)), dma((2,)), dma((2,)), dma, dma,
            ],
            compiler_params=pltpu.CompilerParams(collective_id=0, has_side_effects=True),
        )(neighbours.T, queries, keys_stale, keys_now, values_stale, values_now)

    in_specs = (P(("grp", "reg"), None),) * 5 + (P("grp", None),)
    return jax.shard_map(
        on_device, mesh=mesh, in_specs=in_specs, out_specs=P(("grp", "reg"), None), check_vma=False
    )
```

```python
import functools

import jax
import jax.numpy as jnp
from jax import lax
from jax.experimental import pallas as pl
from jax.experimental.pallas import tpu as pltpu
from jax.sharding import PartitionSpec as P

HD = 128
MESH = pl.DeviceIdType.MESH
LOG2E = 1.4426950408889634
LOW = -1e30
GROUP = 4
Q, KS, KN, VS, VN = range(5)
ORDER = (
    (0, 1), (0, 3), (1, 0), (3, 0), (1, 1), (3, 3), (1, 3), (3, 1),
    (2, 0), (0, 2), (2, 1), (3, 2), (2, 3), (1, 2), (2, 2),
)


def kernel(side, slots, nb_ref, q_ref, ks_ref, kn_ref, vs_ref, vn_ref, out_ref,
           stage, in_q, in_ks, in_kn, in_vs, in_vn, ps, pn, mb, lb, osum, outbox,
           load_sem, send_sem, recv_sem, fsend_sem, frecv_sem, osend_sem, orecv_sem):
    n = side * side
    half = n // 2
    rows = q_ref.shape[0]
    core = lax.rem(lax.axis_index("grp"), 2)
    me = lax.axis_index("reg")
    y, x = me // side, lax.rem(me, side)
    part = y // 2
    scale = HD ** -0.5 * LOG2E
    args = (q_ref, ks_ref, kn_ref, vs_ref, vn_ref)
    inbox = (in_q, in_ks, in_kn, in_vs, in_vn)

    def role(yy, xx):
        whole = lax.rem(xx + core, 2) == 0
        outer = (yy // (side - 1) + (side - 1 - yy) // (side - 1)).astype(jnp.int32)
        return whole, jnp.where(whole, yy * 2 + xx // 2, n // 2 + 2 * outer + xx // 2)

    whole, my_head = role(y, x)
    shared = jnp.logical_not(whole)
    partner = (side - 1 - y) * side + x
    edge = jnp.logical_or(me == half - 1, me == half)
    first = jnp.where(whole, 0, part * half)
    count = jnp.where(whole, n, half)

    def cols(h):
        return pl.ds(pl.multiple_of(h * HD, HD), HD)

    for t, ref in enumerate(args):
        pltpu.make_async_copy(ref, stage.at[t], load_sem.at[t]).start()
    for t, ref in enumerate(args):
        pltpu.make_async_copy(ref.at[:, cols(my_head)], inbox[t].at[me], recv_sem.at[t]).start()

    barrier = pltpu.get_barrier_semaphore()
    for o in range(1, n):
        pl.semaphore_signal(barrier, inc=1, device_id={"reg": lax.rem(me + o, n)}, device_id_type=MESH)
    pl.semaphore_wait(barrier, n - 1)

    def send(t):
        pltpu.make_async_copy(args[t], stage.at[t], load_sem.at[t]).wait()
        for dy, dx in ORDER:
            yy, xx = lax.rem(y + dy, side), lax.rem(x + dx, side)
            takes, head = role(yy, xx)
            takes = jnp.logical_or(takes, yy // 2 == part)
            if t in (KN, VN):
                takes = jnp.logical_or(takes, edge)

            @pl.when(takes)
            def _():
                pltpu.make_async_remote_copy(
                    src_ref=stage.at[t, :, cols(head)],
                    dst_ref=inbox[t].at[me],
                    send_sem=send_sem.at[t],
                    recv_sem=recv_sem.at[t],
                    device_id={"reg": yy * side + xx},
                    device_id_type=MESH,
                ).start()

    def wait(sem, tiles):
        some = in_q.at[pl.ds(0, tiles)]
        pltpu.make_async_copy(some, some, sem).wait()

    most = n - 1 - side

    def sent(t):
        if t in (KN, VN):
            @pl.when(edge)
            def _():
                wait(send_sem.at[t], n - 1)

            @pl.when(jnp.logical_not(edge))
            def _():
                wait(send_sem.at[t], most)
        else:
            wait(send_sem.at[t], most)

    def arrived(t):
        @pl.when(whole)
        def _():
            wait(recv_sem.at[t], n)

        @pl.when(shared)
        def _():
            wait(recv_sem.at[t], half + 1 if t in (KN, VN) else half)

    def forward(t):
        mine = inbox[t].at[pl.ds(part * half, half)]
        return pltpu.make_async_remote_copy(
            src_ref=mine,
            dst_ref=mine,
            send_sem=fsend_sem.at[t // 2],
            recv_sem=frecv_sem.at[t // 2],
            device_id={"reg": partner},
            device_id_type=MESH,
        )

    def pass_on(t):
        arrived(t)

        @pl.when(shared)
        def _():
            forward(t).start()

    def passed(t):
        @pl.when(shared)
        def _():
            wait(frecv_sem.at[t // 2], half)

    send(KS)
    send(Q)
    sent(KS)
    send(KN)
    pass_on(KS)
    sent(Q)
    send(VS)
    arrived(Q)
    passed(KS)

    def softmax_parts(scores):
        peak = jnp.max(scores, axis=-1, keepdims=True)
        weights = jnp.exp2((scores - peak) * scale)
        total = jnp.sum(weights, axis=-1, keepdims=True)
        return peak, weights, total

    def each(one, *outs):
        def step(i, _):
            at = [first + i * GROUP + k for k in range(GROUP)]
            got = [one(r) for r in at]
            for r, values in zip(at, got):
                for ref, value in zip(outs, values):
                    ref[r] = value
            return 0

        lax.fori_loop(0, count // GROUP, step, 0)

    def stale_scores(r):
        idx = [nb_ref[s, r] for s in range(slots)]
        keys = jnp.concatenate([in_ks[jnp.maximum(i, 0)] for i in idx], axis=0)
        sc = lax.dot_general(in_q[r], keys, (((1,), (1,)), ((), ())), preferred_element_type=jnp.float32)
        sc = jnp.concatenate(
            [jnp.where(i >= 0, sc[:, s * rows:(s + 1) * rows], LOW) for s, i in enumerate(idx)], axis=1)
        peak, weights, total = softmax_parts(sc)
        return weights.astype(jnp.bfloat16), jnp.broadcast_to(peak, (rows, HD)), jnp.broadcast_to(total, (rows, HD))

    each(stale_scores, ps, mb, lb)
    sent(KN)
    send(VN)
    pass_on(VS)
    arrived(KN)

    def around(ref, r):
        return jnp.concatenate([ref[jnp.maximum(r - 1, 0)], ref[r], ref[jnp.minimum(r + 1, n - 1)]], axis=0)

    def local_scores(r):
        sc = lax.dot_general(
            in_q[r], around(in_kn, r), (((1,), (1,)), ((), ())), preferred_element_type=jnp.float32)
        sc = jnp.concatenate([
            jnp.where(r > 0, sc[:, :rows], LOW),
            sc[:, rows:2 * rows],
            jnp.where(r < n - 1, sc[:, 2 * rows:], LOW)], axis=1)
        peak, weights, total = softmax_parts(sc)
        peak_s, total_s = mb[r], lb[r]
        peak = jnp.broadcast_to(peak, (rows, HD))
        top = jnp.maximum(peak, peak_s)
        keep_n = jnp.exp2((peak - top) * scale)
        keep_s = jnp.exp2((peak_s - top) * scale)
        inv = 1.0 / (keep_n * total + keep_s * total_s)
        wn = keep_n * inv
        return (weights * jnp.concatenate([wn, wn, wn], axis=1)).astype(jnp.bfloat16), keep_s * inv

    each(local_scores, pn, lb)
    passed(VS)

    def stale_values(r):
        values = jnp.concatenate([in_vs[jnp.maximum(nb_ref[s, r], 0)] for s in range(slots)], axis=0)
        return (lb[r] * jnp.dot(ps[r], values, preferred_element_type=jnp.float32),)

    each(stale_values, osum)
    arrived(VN)

    def tile(r):
        return (osum[r] + jnp.dot(pn[r], around(in_vn, r), preferred_element_type=jnp.float32)).astype(jnp.bfloat16)

    def finish(o, _):
        r = first + lax.rem(me - first + o, count)
        outbox[r] = tile(r)
        pltpu.make_async_remote_copy(
            src_ref=outbox.at[r],
            dst_ref=out_ref.at[:, cols(my_head)],
            send_sem=osend_sem,
            recv_sem=orecv_sem,
            device_id={"reg": r},
            device_id_type=MESH,
        ).start()
        return 0

    lax.fori_loop(1, count, finish, 0)
    out_ref[:, cols(my_head)] = tile(me)

    sent(VS)
    sent(VN)

    @pl.when(whole)
    def _():
        wait(osend_sem, n - 1)

    @pl.when(shared)
    def _():
        wait(osend_sem, half - 1)
        wait(fsend_sem.at[0], half)
        wait(fsend_sem.at[1], half)

    wait(orecv_sem, most)


def solution(mesh):
    n = mesh.shape["reg"]
    side = 4
    assert side * side == n

    def on_device(queries, keys_now, values_now, keys_stale, values_stale, neighbours):
        rows, width = queries.shape
        slots = neighbours.shape[1]
        assert width == (n - side) * HD
        any_spec = pl.BlockSpec(memory_space=pl.ANY)
        dma = pltpu.SemaphoreType.DMA
        return pl.pallas_call(
            functools.partial(kernel, side, slots),
            out_shape=jax.ShapeDtypeStruct((rows, width), jnp.bfloat16),
            in_specs=[pl.BlockSpec(memory_space=pltpu.SMEM)] + [any_spec] * 5,
            out_specs=pl.BlockSpec(memory_space=pltpu.VMEM),
            scratch_shapes=[pltpu.VMEM((5, rows, width), jnp.bfloat16)]
            + [pltpu.VMEM((n, rows, HD), jnp.bfloat16)] * 5
            + [
                pltpu.VMEM((n, rows, slots * rows), jnp.bfloat16),
                pltpu.VMEM((n, rows, 3 * rows), jnp.bfloat16),
                pltpu.VMEM((n, rows, HD), jnp.float32),
                pltpu.VMEM((n, rows, HD), jnp.float32),
                pltpu.VMEM((n, rows, HD), jnp.float32),
                pltpu.VMEM((n, rows, HD), jnp.bfloat16),
                dma((5,)), dma((5,)), dma((5,)), dma((2,)), dma((2,)), dma, dma,
            ],
            compiler_params=pltpu.CompilerParams(collective_id=0, has_side_effects=True, vmem_limit_bytes=20 << 20),
        )(pltpu.with_memory_space_constraint(neighbours.T, pltpu.HBM), *[pltpu.with_memory_space_constraint(a, pltpu.HBM) for a in (queries, keys_stale, keys_now, values_stale, values_now)])

    in_specs = (P(("grp", "reg"), None),) * 5 + (P("grp", None),)
    return jax.shard_map(
        on_device, mesh=mesh, in_specs=in_specs, out_specs=P(("grp", "reg"), None), check_vma=False
    )
```

```python
import functools

import jax
import jax.numpy as jnp
from jax import lax
from jax.experimental import pallas as pl
from jax.experimental.pallas import tpu as pltpu
from jax.sharding import PartitionSpec as P

HD = 128
MESH = pl.DeviceIdType.MESH
LOG2E = 1.4426950408889634
LOW = -1e30
GROUP = 4
Q, KS, KN, VS, VN = range(5)
ORDER = (
    (0, 1), (0, 3), (1, 0), (3, 0), (1, 1), (3, 3), (1, 3), (3, 1),
    (2, 0), (0, 2), (2, 1), (3, 2), (2, 3), (1, 2), (2, 2),
)
FURTHER = ((1, 1), (2, 1), (2, 2))


def kernel(side, slots, nb_ref, q_ref, ks_ref, kn_ref, vs_ref, vn_ref, out_ref,
           stage, in_q, in_ks, in_kn, in_vs, in_vn, ps, pn, mb, lb, osum, outbox,
           load_sem, send_sem, recv_sem, fsend_sem, frecv_sem, osend_sem, orecv_sem, greet_sem):
    n = side * side
    half = n // 2
    rows = q_ref.shape[0]
    core = lax.rem(lax.axis_index("grp"), 2)
    me = lax.axis_index("reg")
    y, x = me // side, lax.rem(me, side)
    part = y // 2
    scale = HD ** -0.5 * LOG2E
    args = (q_ref, ks_ref, kn_ref, vs_ref, vn_ref)
    inbox = (in_q, in_ks, in_kn, in_vs, in_vn)

    def role(yy, xx):
        whole = lax.rem(xx + core, 2) == 0
        outer = (yy // (side - 1) + (side - 1 - yy) // (side - 1)).astype(jnp.int32)
        return whole, jnp.where(whole, yy * 2 + xx // 2, n // 2 + 2 * outer + xx // 2)

    whole, my_head = role(y, x)
    shared = jnp.logical_not(whole)
    partner = (side - 1 - y) * side + x
    edge = jnp.logical_or(me == half - 1, me == half)
    first = jnp.where(whole, 0, part * half)
    count = jnp.where(whole, n, half)

    def cols(h):
        return pl.ds(pl.multiple_of(h * HD, HD), HD)

    for t, ref in enumerate(args):
        pltpu.make_async_copy(ref, stage.at[t], load_sem.at[t]).start()
    for t, ref in enumerate(args):
        pltpu.make_async_copy(ref.at[:, cols(my_head)], inbox[t].at[me], recv_sem.at[t]).start()

    def greet(sem):
        for dy, dx in ORDER[:4]:
            there = lax.rem(y + dy, side) * side + lax.rem(x + dx, side)
            pl.semaphore_signal(sem, inc=1, device_id={"reg": there}, device_id_type=MESH)
        pl.semaphore_wait(sem, 4)

    greet(pltpu.get_barrier_semaphore())

    def send(t, greeting=False):
        pltpu.make_async_copy(args[t], stage.at[t], load_sem.at[t]).wait()
        for dy, dx in ORDER:
            if greeting and (dy, dx) in FURTHER:
                greet(greet_sem.at[FURTHER.index((dy, dx))])
            yy, xx = lax.rem(y + dy, side), lax.rem(x + dx, side)
            takes, head = role(yy, xx)
            takes = jnp.logical_or(takes, yy // 2 == part)
            if t in (KN, VN):
                takes = jnp.logical_or(takes, edge)

            @pl.when(takes)
            def _():
                pltpu.make_async_remote_copy(
                    src_ref=stage.at[t, :, cols(head)],
                    dst_ref=inbox[t].at[me],
                    send_sem=send_sem.at[t],
                    recv_sem=recv_sem.at[t],
                    device_id={"reg": yy * side + xx},
                    device_id_type=MESH,
                ).start()

    def wait(sem, tiles):
        some = in_q.at[pl.ds(0, tiles)]
        pltpu.make_async_copy(some, some, sem).wait()

    most = n - 1 - side

    def sent(t):
        if t in (KN, VN):
            @pl.when(edge)
            def _():
                wait(send_sem.at[t], n - 1)

            @pl.when(jnp.logical_not(edge))
            def _():
                wait(send_sem.at[t], most)
        else:
            wait(send_sem.at[t], most)

    def arrived(t):
        @pl.when(whole)
        def _():
            wait(recv_sem.at[t], n)

        @pl.when(shared)
        def _():
            wait(recv_sem.at[t], half + 1 if t in (KN, VN) else half)

    def forward(t):
        mine = inbox[t].at[pl.ds(part * half, half)]
        return pltpu.make_async_remote_copy(
            src_ref=mine,
            dst_ref=mine,
            send_sem=fsend_sem.at[t // 2],
            recv_sem=frecv_sem.at[t // 2],
            device_id={"reg": partner},
            device_id_type=MESH,
        )

    def pass_on(t):
        arrived(t)

        @pl.when(shared)
        def _():
            forward(t).start()

    def passed(t):
        @pl.when(shared)
        def _():
            wait(frecv_sem.at[t // 2], half)

    send(KS, greeting=True)
    send(Q)
    sent(KS)
    send(KN)
    pass_on(KS)
    sent(Q)
    send(VS)
    arrived(Q)
    passed(KS)

    def softmax_parts(scores):
        peak = jnp.max(scores, axis=-1, keepdims=True)
        weights = jnp.exp2((scores - peak) * scale)
        total = jnp.sum(weights, axis=-1, keepdims=True)
        return peak, weights, total

    def each(one, *outs):
        def step(i, _):
            at = [first + i * GROUP + k for k in range(GROUP)]
            got = [one(r) for r in at]
            for r, values in zip(at, got):
                for ref, value in zip(outs, values):
                    ref[r] = value
            return 0

        lax.fori_loop(0, count // GROUP, step, 0)

    def stale_scores(r):
        idx = [nb_ref[s, r] for s in range(slots)]
        keys = jnp.concatenate([in_ks[jnp.maximum(i, 0)] for i in idx], axis=0)
        sc = lax.dot_general(in_q[r], keys, (((1,), (1,)), ((), ())), preferred_element_type=jnp.float32)
        sc = jnp.concatenate(
            [jnp.where(i >= 0, sc[:, s * rows:(s + 1) * rows], LOW) for s, i in enumerate(idx)], axis=1)
        peak, weights, total = softmax_parts(sc)
        return weights.astype(jnp.bfloat16), jnp.broadcast_to(peak, (rows, HD)), jnp.broadcast_to(total, (rows, HD))

    each(stale_scores, ps, mb, lb)
    sent(KN)
    send(VN)
    pass_on(VS)
    arrived(KN)

    def around(ref, r):
        return jnp.concatenate([ref[jnp.maximum(r - 1, 0)], ref[r], ref[jnp.minimum(r + 1, n - 1)]], axis=0)

    def local_scores(r):
        sc = lax.dot_general(
            in_q[r], around(in_kn, r), (((1,), (1,)), ((), ())), preferred_element_type=jnp.float32)
        sc = jnp.concatenate([
            jnp.where(r > 0, sc[:, :rows], LOW),
            sc[:, rows:2 * rows],
            jnp.where(r < n - 1, sc[:, 2 * rows:], LOW)], axis=1)
        peak, weights, total = softmax_parts(sc)
        peak_s, total_s = mb[r], lb[r]
        peak = jnp.broadcast_to(peak, (rows, HD))
        top = jnp.maximum(peak, peak_s)
        keep_n = jnp.exp2((peak - top) * scale)
        keep_s = jnp.exp2((peak_s - top) * scale)
        inv = 1.0 / (keep_n * total + keep_s * total_s)
        wn = keep_n * inv
        return (weights * jnp.concatenate([wn, wn, wn], axis=1)).astype(jnp.bfloat16), keep_s * inv

    each(local_scores, pn, lb)
    passed(VS)

    def stale_values(r):
        values = jnp.concatenate([in_vs[jnp.maximum(nb_ref[s, r], 0)] for s in range(slots)], axis=0)
        return (lb[r] * jnp.dot(ps[r], values, preferred_element_type=jnp.float32),)

    each(stale_values, osum)
    arrived(VN)

    def tile(r):
        return (osum[r] + jnp.dot(pn[r], around(in_vn, r), preferred_element_type=jnp.float32)).astype(jnp.bfloat16)

    def give(r):
        outbox[r] = tile(r)
        pltpu.make_async_remote_copy(
            src_ref=outbox.at[r],
            dst_ref=out_ref.at[:, cols(my_head)],
            send_sem=osend_sem,
            recv_sem=orecv_sem,
            device_id={"reg": r},
            device_id_type=MESH,
        ).start()

    @pl.when(jnp.logical_and(first == 0, me != 0))
    def _():
        give(0)

    def finish(o, _):
        r = first + lax.rem(me - first + o, count)

        @pl.when(r != 0)
        def _():
            give(r)

        return 0

    lax.fori_loop(1, count, finish, 0)
    out_ref[:, cols(my_head)] = tile(me)

    sent(VS)
    sent(VN)

    @pl.when(whole)
    def _():
        wait(osend_sem, n - 1)

    @pl.when(shared)
    def _():
        wait(osend_sem, half - 1)
        wait(fsend_sem.at[0], half)
        wait(fsend_sem.at[1], half)

    wait(orecv_sem, most)


def solution(mesh):
    n = mesh.shape["reg"]
    side = 4
    assert side * side == n

    def on_device(queries, keys_now, values_now, keys_stale, values_stale, neighbours):
        rows, width = queries.shape
        slots = neighbours.shape[1]
        assert width == (n - side) * HD
        any_spec = pl.BlockSpec(memory_space=pl.ANY)
        dma = pltpu.SemaphoreType.DMA
        return pl.pallas_call(
            functools.partial(kernel, side, slots),
            out_shape=jax.ShapeDtypeStruct((rows, width), jnp.bfloat16),
            in_specs=[pl.BlockSpec(memory_space=pltpu.SMEM)] + [any_spec] * 5,
            out_specs=pl.BlockSpec(memory_space=pltpu.VMEM),
            scratch_shapes=[pltpu.VMEM((5, rows, width), jnp.bfloat16)]
            + [pltpu.VMEM((n, rows, HD), jnp.bfloat16)] * 5
            + [
                pltpu.VMEM((n, rows, slots * rows), jnp.bfloat16),
                pltpu.VMEM((n, rows, 3 * rows), jnp.bfloat16),
                pltpu.VMEM((n, rows, HD), jnp.float32),
                pltpu.VMEM((n, rows, HD), jnp.float32),
                pltpu.VMEM((n, rows, HD), jnp.float32),
                pltpu.VMEM((n, rows, HD), jnp.bfloat16),
                dma((5,)), dma((5,)), dma((5,)), dma((2,)), dma((2,)), dma, dma, pltpu.SemaphoreType.REGULAR((3,)),
            ],
            compiler_params=pltpu.CompilerParams(collective_id=0, has_side_effects=True, vmem_limit_bytes=20 << 20),
        )(pltpu.with_memory_space_constraint(neighbours.T, pltpu.HBM), *[pltpu.with_memory_space_constraint(a, pltpu.HBM) for a in (queries, keys_stale, keys_now, values_stale, values_now)])

    in_specs = (P(("grp", "reg"), None),) * 5 + (P("grp", None),)
    return jax.shard_map(
        on_device, mesh=mesh, in_specs=in_specs, out_specs=P(("grp", "reg"), None), check_vma=False
    )
```

```python
import functools

import jax
import jax.numpy as jnp
from jax import lax
from jax.experimental import pallas as pl
from jax.experimental.pallas import tpu as pltpu
from jax.sharding import PartitionSpec as P

HD = 128
MESH = pl.DeviceIdType.MESH
LOG2E = 1.4426950408889634
LOW = -1e30
GROUP = 4
Q, KS, KN, VS, VN = range(5)
ORDER = (
    (0, 1), (0, 3), (1, 0), (3, 0), (1, 1), (3, 3), (1, 3), (3, 1),
    (2, 0), (0, 2), (2, 1), (3, 2), (2, 3), (1, 2), (2, 2),
)
FURTHER = ((1, 1), (2, 1), (2, 2))


def kernel(side, slots, nb_ref, q_ref, ks_ref, kn_ref, vs_ref, vn_ref, out_ref,
           stage, in_q, in_ks, in_kn, in_vs, in_vn, ps, pn, mb, lb, osum, outbox,
           load_sem, send_sem, recv_sem, fsend_sem, frecv_sem, osend_sem, orecv_sem, greet_sem):
    n = side * side
    half = n // 2
    rows = q_ref.shape[0]
    core = lax.rem(lax.axis_index("grp"), 2)
    me = lax.axis_index("reg")
    y, x = me // side, lax.rem(me, side)
    part = y // 2
    scale = HD ** -0.5 * LOG2E
    args = (q_ref, ks_ref, kn_ref, vs_ref, vn_ref)
    inbox = (in_q, in_ks, in_kn, in_vs, in_vn)

    def role(yy, xx):
        whole = lax.rem(xx + core, 2) == 0
        outer = (yy // (side - 1) + (side - 1 - yy) // (side - 1)).astype(jnp.int32)
        return whole, jnp.where(whole, yy * 2 + xx // 2, n // 2 + 2 * outer + xx // 2)

    whole, my_head = role(y, x)
    shared = jnp.logical_not(whole)
    partner = (side - 1 - y) * side + x
    edge = jnp.logical_or(me == half - 1, me == half)
    first = jnp.where(whole, 0, part * half)
    count = jnp.where(whole, n, half)

    def cols(h):
        return pl.ds(pl.multiple_of(h * HD, HD), HD)

    def hail(sem):
        for dy, dx in ORDER[:4]:
            there = lax.rem(y + dy, side) * side + lax.rem(x + dx, side)
            pl.semaphore_signal(sem, inc=1, device_id={"reg": there}, device_id_type=MESH)

    def greet(sem):
        hail(sem)
        pl.semaphore_wait(sem, 4)

    barrier = pltpu.get_barrier_semaphore()
    hail(barrier)
    for t in (KS, Q, KN, VS, VN):
        pltpu.make_async_copy(args[t], stage.at[t], load_sem.at[t]).start()
    for t, ref in enumerate(args):
        pltpu.make_async_copy(ref.at[:, cols(my_head)], inbox[t].at[me], recv_sem.at[t]).start()

    pl.semaphore_wait(barrier, 4)

    def send(t, greeting=False):
        pltpu.make_async_copy(args[t], stage.at[t], load_sem.at[t]).wait()
        for dy, dx in ORDER:
            if greeting and (dy, dx) in FURTHER:
                greet(greet_sem.at[FURTHER.index((dy, dx))])
            yy, xx = lax.rem(y + dy, side), lax.rem(x + dx, side)
            takes, head = role(yy, xx)
            takes = jnp.logical_or(takes, yy // 2 == part)
            if t in (KN, VN):
                takes = jnp.logical_or(takes, edge)

            @pl.when(takes)
            def _():
                pltpu.make_async_remote_copy(
                    src_ref=stage.at[t, :, cols(head)],
                    dst_ref=inbox[t].at[me],
                    send_sem=send_sem.at[t],
                    recv_sem=recv_sem.at[t],
                    device_id={"reg": yy * side + xx},
                    device_id_type=MESH,
                ).start()

    def wait(sem, tiles):
        some = in_q.at[pl.ds(0, tiles)]
        pltpu.make_async_copy(some, some, sem).wait()

    most = n - 1 - side

    def sent(t):
        if t in (KN, VN):
            @pl.when(edge)
            def _():
                wait(send_sem.at[t], n - 1)

            @pl.when(jnp.logical_not(edge))
            def _():
                wait(send_sem.at[t], most)
        else:
            wait(send_sem.at[t], most)

    def arrived(t):
        @pl.when(whole)
        def _():
            wait(recv_sem.at[t], n)

        @pl.when(shared)
        def _():
            wait(recv_sem.at[t], half + 1 if t in (KN, VN) else half)

    def forward(t):
        mine = inbox[t].at[pl.ds(part * half, half)]
        return pltpu.make_async_remote_copy(
            src_ref=mine,
            dst_ref=mine,
            send_sem=fsend_sem.at[t // 2],
            recv_sem=frecv_sem.at[t // 2],
            device_id={"reg": partner},
            device_id_type=MESH,
        )

    def pass_on(t):
        arrived(t)

        @pl.when(shared)
        def _():
            forward(t).start()

    def passed(t):
        @pl.when(shared)
        def _():
            wait(frecv_sem.at[t // 2], half)

    send(KS, greeting=True)
    send(Q)
    sent(KS)
    send(VS)
    pass_on(KS)
    sent(Q)
    send(KN)
    arrived(Q)
    passed(KS)

    def softmax_parts(scores):
        peak = jnp.max(scores, axis=-1, keepdims=True)
        weights = jnp.exp2((scores - peak) * scale)
        total = jnp.sum(weights, axis=-1, keepdims=True)
        return peak, weights, total

    def each(one, *outs):
        def step(i, _):
            at = [first + i * GROUP + k for k in range(GROUP)]
            got = [one(r) for r in at]
            for r, values in zip(at, got):
                for ref, value in zip(outs, values):
                    ref[r] = value
            return 0

        lax.fori_loop(0, count // GROUP, step, 0)

    def stale_scores(r):
        idx = [nb_ref[s, r] for s in range(slots)]
        keys = jnp.concatenate([in_ks[jnp.maximum(i, 0)] for i in idx], axis=0)
        sc = lax.dot_general(in_q[r], keys, (((1,), (1,)), ((), ())), preferred_element_type=jnp.float32)
        sc = jnp.concatenate(
            [jnp.where(i >= 0, sc[:, s * rows:(s + 1) * rows], LOW) for s, i in enumerate(idx)], axis=1)
        peak, weights, total = softmax_parts(sc)
        return weights.astype(jnp.bfloat16), jnp.broadcast_to(peak, (rows, HD)), jnp.broadcast_to(total, (rows, HD))

    each(stale_scores, ps, mb, lb)
    send(VN)
    pass_on(VS)
    sent(KN)
    arrived(KN)

    def around(ref, r):
        return jnp.concatenate([ref[jnp.maximum(r - 1, 0)], ref[r], ref[jnp.minimum(r + 1, n - 1)]], axis=0)

    def local_scores(r):
        sc = lax.dot_general(
            in_q[r], around(in_kn, r), (((1,), (1,)), ((), ())), preferred_element_type=jnp.float32)
        sc = jnp.concatenate([
            jnp.where(r > 0, sc[:, :rows], LOW),
            sc[:, rows:2 * rows],
            jnp.where(r < n - 1, sc[:, 2 * rows:], LOW)], axis=1)
        peak, weights, total = softmax_parts(sc)
        peak_s, total_s = mb[r], lb[r]
        peak = jnp.broadcast_to(peak, (rows, HD))
        top = jnp.maximum(peak, peak_s)
        keep_n = jnp.exp2((peak - top) * scale)
        keep_s = jnp.exp2((peak_s - top) * scale)
        inv = 1.0 / (keep_n * total + keep_s * total_s)
        wn = keep_n * inv
        return (weights * jnp.concatenate([wn, wn, wn], axis=1)).astype(jnp.bfloat16), keep_s * inv

    each(local_scores, pn, lb)
    passed(VS)

    def stale_values(r):
        values = jnp.concatenate([in_vs[jnp.maximum(nb_ref[s, r], 0)] for s in range(slots)], axis=0)
        return (lb[r] * jnp.dot(ps[r], values, preferred_element_type=jnp.float32),)

    each(stale_values, osum)
    arrived(VN)

    def tile(r):
        return (osum[r] + jnp.dot(pn[r], around(in_vn, r), preferred_element_type=jnp.float32)).astype(jnp.bfloat16)

    def give(r):
        outbox[r] = tile(r)
        pltpu.make_async_remote_copy(
            src_ref=outbox.at[r],
            dst_ref=out_ref.at[:, cols(my_head)],
            send_sem=osend_sem,
            recv_sem=orecv_sem,
            device_id={"reg": r},
            device_id_type=MESH,
        ).start()

    @pl.when(jnp.logical_and(first == 0, me != 0))
    def _():
        give(0)

    def finish(o, _):
        r = first + lax.rem(me - first + o, count)

        @pl.when(r != 0)
        def _():
            give(r)

        return 0

    lax.fori_loop(1, count, finish, 0)
    out_ref[:, cols(my_head)] = tile(me)

    sent(VS)
    sent(VN)

    @pl.when(whole)
    def _():
        wait(osend_sem, n - 1)

    @pl.when(shared)
    def _():
        wait(osend_sem, half - 1)
        wait(fsend_sem.at[0], half)
        wait(fsend_sem.at[1], half)

    wait(orecv_sem, most)


def solution(mesh):
    n = mesh.shape["reg"]
    side = 4
    assert side * side == n

    def on_device(queries, keys_now, values_now, keys_stale, values_stale, neighbours):
        rows, width = queries.shape
        slots = neighbours.shape[1]
        assert width == (n - side) * HD
        any_spec = pl.BlockSpec(memory_space=pl.ANY)
        dma = pltpu.SemaphoreType.DMA
        return pl.pallas_call(
            functools.partial(kernel, side, slots),
            out_shape=jax.ShapeDtypeStruct((rows, width), jnp.bfloat16),
            in_specs=[pl.BlockSpec(memory_space=pltpu.SMEM)] + [any_spec] * 5,
            out_specs=pl.BlockSpec(memory_space=pltpu.VMEM),
            scratch_shapes=[pltpu.VMEM((5, rows, width), jnp.bfloat16)]
            + [pltpu.VMEM((n, rows, HD), jnp.bfloat16)] * 5
            + [
                pltpu.VMEM((n, rows, slots * rows), jnp.bfloat16),
                pltpu.VMEM((n, rows, 3 * rows), jnp.bfloat16),
                pltpu.VMEM((n, rows, HD), jnp.float32),
                pltpu.VMEM((n, rows, HD), jnp.float32),
                pltpu.VMEM((n, rows, HD), jnp.float32),
                pltpu.VMEM((n, rows, HD), jnp.bfloat16),
                dma((5,)), dma((5,)), dma((5,)), dma((2,)), dma((2,)), dma, dma, pltpu.SemaphoreType.REGULAR((3,)),
            ],
            compiler_params=pltpu.CompilerParams(collective_id=0, has_side_effects=True, vmem_limit_bytes=20 << 20),
        )(pltpu.with_memory_space_constraint(neighbours.T, pltpu.HBM), *[pltpu.with_memory_space_constraint(a, pltpu.HBM) for a in (queries, keys_stale, keys_now, values_stale, values_now)])

    in_specs = (P(("grp", "reg"), None),) * 5 + (P("grp", None),)
    return jax.shard_map(
        on_device, mesh=mesh, in_specs=in_specs, out_specs=P(("grp", "reg"), None), check_vma=False
    )
```

```python
import functools

import jax
import jax.numpy as jnp
from jax import lax
from jax.experimental import pallas as pl
from jax.experimental.pallas import tpu as pltpu
from jax.sharding import PartitionSpec as P

HD = 128
MESH = pl.DeviceIdType.MESH
LOG2E = 1.4426950408889634
LOW = -1e30
GROUP = 8
Q, KS, KN, VS, VN = range(5)
ORDER = (
    (0, 1), (0, 3), (1, 0), (3, 0), (1, 1), (3, 3), (1, 3), (3, 1),
    (2, 0), (0, 2), (2, 1), (3, 2), (2, 3), (1, 2), (2, 2),
)
FURTHER = ((1, 1), (2, 1), (2, 2))


def kernel(side, slots, nb_ref, q_ref, ks_ref, kn_ref, vs_ref, vn_ref, out_ref,
           stage, in_q, in_ks, in_kn, in_vs, in_vn, ps, pn, mb, lb, osum, outbox,
           load_sem, send_sem, recv_sem, fsend_sem, frecv_sem, osend_sem, orecv_sem, greet_sem):
    n = side * side
    half = n // 2
    rows = q_ref.shape[0]
    core = lax.rem(lax.axis_index("grp"), 2)
    me = lax.axis_index("reg")
    y, x = me // side, lax.rem(me, side)
    part = y // 2
    scale = HD ** -0.5 * LOG2E
    args = (q_ref, ks_ref, kn_ref, vs_ref, vn_ref)
    inbox = (in_q, in_ks, in_kn, in_vs, in_vn)

    def role(yy, xx):
        whole = lax.rem(xx + core, 2) == 0
        outer = (yy // (side - 1) + (side - 1 - yy) // (side - 1)).astype(jnp.int32)
        return whole, jnp.where(whole, yy * 2 + xx // 2, n // 2 + 2 * outer + xx // 2)

    whole, my_head = role(y, x)
    shared = jnp.logical_not(whole)
    partner = (side - 1 - y) * side + x
    edge = jnp.logical_or(me == half - 1, me == half)
    first = jnp.where(whole, 0, part * half)
    count = jnp.where(whole, n, half)

    def cols(h):
        return pl.ds(pl.multiple_of(h * HD, HD), HD)

    def hail(sem):
        for dy, dx in ORDER[:4]:
            there = lax.rem(y + dy, side) * side + lax.rem(x + dx, side)
            pl.semaphore_signal(sem, inc=1, device_id={"reg": there}, device_id_type=MESH)

    def greet(sem):
        hail(sem)
        pl.semaphore_wait(sem, 4)

    barrier = pltpu.get_barrier_semaphore()
    hail(barrier)
    for t in (KS, Q, KN, VS, VN):
        pltpu.make_async_copy(args[t], stage.at[t], load_sem.at[t]).start()
    for t, ref in enumerate(args):
        pltpu.make_async_copy(ref.at[:, cols(my_head)], inbox[t].at[me], recv_sem.at[t]).start()

    pl.semaphore_wait(barrier, 4)

    def send(t, greeting=False):
        pltpu.make_async_copy(args[t], stage.at[t], load_sem.at[t]).wait()
        for dy, dx in ORDER:
            if greeting and (dy, dx) in FURTHER:
                greet(greet_sem.at[FURTHER.index((dy, dx))])
            yy, xx = lax.rem(y + dy, side), lax.rem(x + dx, side)
            takes, head = role(yy, xx)
            takes = jnp.logical_or(takes, yy // 2 == part)
            if t in (KN, VN):
                takes = jnp.logical_or(takes, edge)

            @pl.when(takes)
            def _():
                pltpu.make_async_remote_copy(
                    src_ref=stage.at[t, :, cols(head)],
                    dst_ref=inbox[t].at[me],
                    send_sem=send_sem.at[t],
                    recv_sem=recv_sem.at[t],
                    device_id={"reg": yy * side + xx},
                    device_id_type=MESH,
                ).start()

    def wait(sem, tiles):
        some = in_q.at[pl.ds(0, tiles)]
        pltpu.make_async_copy(some, some, sem).wait()

    most = n - 1 - side

    def sent(t):
        if t in (KN, VN):
            @pl.when(edge)
            def _():
                wait(send_sem.at[t], n - 1)

            @pl.when(jnp.logical_not(edge))
            def _():
                wait(send_sem.at[t], most)
        else:
            wait(send_sem.at[t], most)

    def arrived(t):
        @pl.when(whole)
        def _():
            wait(recv_sem.at[t], n)

        @pl.when(shared)
        def _():
            wait(recv_sem.at[t], half + 1 if t in (KN, VN) else half)

    def forward(t):
        mine = inbox[t].at[pl.ds(part * half, half)]
        return pltpu.make_async_remote_copy(
            src_ref=mine,
            dst_ref=mine,
            send_sem=fsend_sem.at[t // 2],
            recv_sem=frecv_sem.at[t // 2],
            device_id={"reg": partner},
            device_id_type=MESH,
        )

    def pass_on(t):
        arrived(t)

        @pl.when(shared)
        def _():
            forward(t).start()

    def passed(t):
        @pl.when(shared)
        def _():
            wait(frecv_sem.at[t // 2], half)

    send(KS, greeting=True)
    send(Q)
    sent(KS)
    send(VS)
    pass_on(KS)
    sent(Q)
    send(KN)
    arrived(Q)
    passed(KS)

    def softmax_parts(scores):
        peak = jnp.max(scores, axis=-1, keepdims=True)
        weights = jnp.exp2((scores - peak) * scale)
        total = jnp.sum(weights, axis=-1, keepdims=True)
        return peak, weights, total

    def each(one, *outs):
        def step(i, _):
            at = [first + i * GROUP + k for k in range(GROUP)]
            got = [one(r) for r in at]
            for r, values in zip(at, got):
                for ref, value in zip(outs, values):
                    ref[r] = value
            return 0

        lax.fori_loop(0, count // GROUP, step, 0)

    def stale_scores(r):
        idx = [nb_ref[s, r] for s in range(slots)]
        keys = jnp.concatenate([in_ks[jnp.maximum(i, 0)] for i in idx], axis=0)
        sc = lax.dot_general(in_q[r], keys, (((1,), (1,)), ((), ())), preferred_element_type=jnp.float32)
        sc = jnp.concatenate(
            [jnp.where(i >= 0, sc[:, s * rows:(s + 1) * rows], LOW) for s, i in enumerate(idx)], axis=1)
        peak, weights, total = softmax_parts(sc)
        return weights.astype(jnp.bfloat16), jnp.broadcast_to(peak, (rows, HD)), jnp.broadcast_to(total, (rows, HD))

    each(stale_scores, ps, mb, lb)
    send(VN)
    pass_on(VS)
    sent(KN)
    arrived(KN)

    def around(ref, r):
        return jnp.concatenate([ref[jnp.maximum(r - 1, 0)], ref[r], ref[jnp.minimum(r + 1, n - 1)]], axis=0)

    def local_scores(r):
        sc = lax.dot_general(
            in_q[r], around(in_kn, r), (((1,), (1,)), ((), ())), preferred_element_type=jnp.float32)
        sc = jnp.concatenate([
            jnp.where(r > 0, sc[:, :rows], LOW),
            sc[:, rows:2 * rows],
            jnp.where(r < n - 1, sc[:, 2 * rows:], LOW)], axis=1)
        peak, weights, total = softmax_parts(sc)
        peak_s, total_s = mb[r], lb[r]
        peak = jnp.broadcast_to(peak, (rows, HD))
        top = jnp.maximum(peak, peak_s)
        keep_n = jnp.exp2((peak - top) * scale)
        keep_s = jnp.exp2((peak_s - top) * scale)
        inv = 1.0 / (keep_n * total + keep_s * total_s)
        wn = keep_n * inv
        return (weights * jnp.concatenate([wn, wn, wn], axis=1)).astype(jnp.bfloat16), keep_s * inv

    each(local_scores, pn, lb)
    passed(VS)

    def stale_values(r):
        values = jnp.concatenate([in_vs[jnp.maximum(nb_ref[s, r], 0)] for s in range(slots)], axis=0)
        return (lb[r] * jnp.dot(ps[r], values, preferred_element_type=jnp.float32),)

    each(stale_values, osum)
    arrived(VN)

    def tile(r):
        return (osum[r] + jnp.dot(pn[r], around(in_vn, r), preferred_element_type=jnp.float32)).astype(jnp.bfloat16)

    def give(r):
        outbox[r] = tile(r)
        pltpu.make_async_remote_copy(
            src_ref=outbox.at[r],
            dst_ref=out_ref.at[:, cols(my_head)],
            send_sem=osend_sem,
            recv_sem=orecv_sem,
            device_id={"reg": r},
            device_id_type=MESH,
        ).start()

    @pl.when(jnp.logical_and(first == 0, me != 0))
    def _():
        give(0)

    def finish(o, _):
        r = first + lax.rem(me - first + o, count)

        @pl.when(r != 0)
        def _():
            give(r)

        return 0

    lax.fori_loop(1, count, finish, 0)
    out_ref[:, cols(my_head)] = tile(me)

    sent(VS)
    sent(VN)

    @pl.when(whole)
    def _():
        wait(osend_sem, n - 1)

    @pl.when(shared)
    def _():
        wait(osend_sem, half - 1)
        wait(fsend_sem.at[0], half)
        wait(fsend_sem.at[1], half)

    wait(orecv_sem, most)


def solution(mesh):
    n = mesh.shape["reg"]
    side = 4
    assert side * side == n

    def on_device(queries, keys_now, values_now, keys_stale, values_stale, neighbours):
        rows, width = queries.shape
        slots = neighbours.shape[1]
        assert width == (n - side) * HD
        any_spec = pl.BlockSpec(memory_space=pl.ANY)
        dma = pltpu.SemaphoreType.DMA
        return pl.pallas_call(
            functools.partial(kernel, side, slots),
            out_shape=jax.ShapeDtypeStruct((rows, width), jnp.bfloat16),
            in_specs=[pl.BlockSpec(memory_space=pltpu.SMEM)] + [any_spec] * 5,
            out_specs=pl.BlockSpec(memory_space=pltpu.VMEM),
            scratch_shapes=[pltpu.VMEM((5, rows, width), jnp.bfloat16)]
            + [pltpu.VMEM((n, rows, HD), jnp.bfloat16)] * 5
            + [
                pltpu.VMEM((n, rows, slots * rows), jnp.bfloat16),
                pltpu.VMEM((n, rows, 3 * rows), jnp.bfloat16),
                pltpu.VMEM((n, rows, HD), jnp.float32),
                pltpu.VMEM((n, rows, HD), jnp.float32),
                pltpu.VMEM((n, rows, HD), jnp.float32),
                pltpu.VMEM((n, rows, HD), jnp.bfloat16),
                dma((5,)), dma((5,)), dma((5,)), dma((2,)), dma((2,)), dma, dma, pltpu.SemaphoreType.REGULAR((3,)),
            ],
            compiler_params=pltpu.CompilerParams(collective_id=0, has_side_effects=True, vmem_limit_bytes=20 << 20),
        )(pltpu.with_memory_space_constraint(neighbours.T, pltpu.HBM), *[pltpu.with_memory_space_constraint(a, pltpu.HBM) for a in (queries, keys_stale, keys_now, values_stale, values_now)])

    in_specs = (P(("grp", "reg"), None),) * 5 + (P("grp", None),)
    return jax.shard_map(
        on_device, mesh=mesh, in_specs=in_specs, out_specs=P(("grp", "reg"), None), check_vma=False
    )
```
